128 devices in a mesh: vocab: 32 (over y, x, z_lo), hid: 4 (over z_hi, core).
Axes of the slice: x: 4, y: 4, z: 4 (z_hi: 2, z_lo: 2; z = z_hi * 2 + z_lo), core: 2. Of those that a mesh axis runs over, the one named last changes fastest.
Arguments:
- hidden: bfloat16 [1, 4096, 3584], P(None, 'vocab', 'hid'), may hold values from -30 to 30
- unembed: bfloat16 [3584, 81920], P(None, ('vocab', 'hid')), may hold values from -10 to 10
- labels: int32 [4096], P('vocab'), may hold values from 0 to 81919
Outputs:
- token_loss: float32 [1, 4096], replicated
- layer_loss: float32 [1], replicated
The draws below stay inside these ranges and needn't reach their ends.
All inputs are finite; a program needn't handle non-finite values.
Results may differ from the reference program's by a relative error of at most 0.0003.
Values may be sent and summed in bfloat16 or wider, within the bound.
No kernel may reach another device: no remote copies, remote signals or barrier semaphores. Data moves between devices by JAX's collectives and lax.ppermute only.
A program may use at most 128 MiB of HBM per device.

```python
import math
import jax
import jax.numpy as jnp
import numpy as np
from jax import lax

D = 3584
V = 81920
LAYERS = 1
TOK_DEV = 128
TOKENS = 4096


def draw_hidden(key, part):
    values = jnp.clip(jax.random.normal(jax.random.fold_in(key, 1), (LAYERS, TOKENS, D), jnp.float32), -6.0, 6.0)
    return values.astype(jnp.bfloat16)


def draw_unembed(key, part):
    values = jnp.clip(jax.random.normal(jax.random.fold_in(key, 3), (D, V), jnp.float32), -6.0, 6.0)
    values = values * (3.0 / math.sqrt(D))
    return values.astype(jnp.bfloat16)


def set_ends(result, key, smallest, top_value):
    index_at = [jax.random.randint(jax.random.fold_in(key, axis), (), 0, length) for axis, length in enumerate(result.shape)]
    widest = result.shape.index(max(result.shape))
    next_to = index_at[:widest] + [(index_at[widest] + 1) % result.shape[widest]] + index_at[widest + 1:]
    return result.at[tuple(index_at)].set(smallest).at[tuple(next_to)].set(top_value)


def wide_ids(own_key, shape, number_of, skew):
    loads = [min(1 << octave, number_of + 1 - (1 << octave)) * (1 << 20) // math.isqrt((1 << octave) ** skew) + 1 for octave in range((number_of + 1).bit_length()) if 1 << octave <= number_of]
    scale = 1 + sum(loads) // (1 << 30)
    grid = np.cumsum(np.array([max(1, weight // scale) for weight in loads]))
    pick = jax.random.randint(jax.random.fold_in(own_key, 1), shape, 0, int(grid[len(loads) - 1]))
    start = jnp.left_shift(1, jnp.searchsorted(jnp.asarray(grid, jnp.int32), pick, side="right").astype(jnp.int32))
    rank = start - 1 + jax.random.randint(jax.random.fold_in(own_key, 4), shape, 0, 1 << 30) % jnp.minimum(start, number_of + 1 - start)
    return jax.random.permutation(jax.random.fold_in(own_key, 2), number_of)[rank].astype(jnp.int32)


def setup_inputs(seed: int = 0) -> dict:
    splits = jax.random.split(jax.random.key(seed), 4)
    hidden = draw_hidden(jax.random.fold_in(splits[3], 71), 0)
    unembed = draw_unembed(jax.random.fold_in(splits[3], 71), 0)
    labels = set_ends(wide_ids(splits[2], (TOKENS,), V, 2), jax.random.fold_in(splits[2], 3), 0, V - 1).astype(jnp.int32)
    return dict(hidden=hidden, unembed=unembed, labels=labels)


def reference(hidden, unembed, labels):
    token_rows = hidden.reshape(-1, TOK_DEV, D)
    targets = jnp.tile(labels, LAYERS).reshape(-1, TOK_DEV).astype(jnp.int32)

    def one_block(block_pair):
        row_block, wanted = block_pair
        logits = jnp.dot(row_block, unembed, preferred_element_type=jnp.float32)
        row_peak = jnp.max(logits, axis=-1)
        row_total = jnp.sum(jnp.exp(logits - row_peak[:, None]), axis=-1)
        picked = jnp.take_along_axis(logits, wanted[:, None], axis=-1)[:, 0]
        return row_peak + jnp.log(row_total) - picked

    token_loss = lax.map(one_block, (token_rows, targets)).reshape(LAYERS, TOKENS)
    return token_loss, jnp.mean(token_loss, axis=1)
```

```python
import jax
import jax.numpy as jnp
from jax import lax
from jax.experimental import pallas as pl
from jax.experimental.pallas import tpu as pltpu
from jax.sharding import PartitionSpec as P

AXES = ("vocab", "hid")


def device_number(y, x, z, core):
    return ((y * 4 + x) * 2 + z % 2) * 4 + (z // 2) * 2 + core


def source_pairs(da, db, dz, dc):
    pairs = []
    for y in range(4):
        for x in range(4):
            for z in range(4):
                for core in range(2):
                    dx, dy = (da, db) if core == 0 else (db, da)
                    source = device_number((y + dy) % 4, (x + dx) % 4, (z + dz) % 4, core ^ dc)
                    pairs.append((source, device_number(y, x, z, core)))
    return pairs


def pull(value, da=0, db=0, dz=0, dc=0):
    return lax.ppermute(value, AXES, source_pairs(da, db, dz, dc))


def place():
    vocab, hid = lax.axis_index("vocab"), lax.axis_index("hid")
    y, x, z_lo = vocab // 8, (vocab // 2) % 4, vocab % 2
    z_hi, core = hid // 2, hid % 2
    a, b = jnp.where(core == 0, x, y), jnp.where(core == 0, y, x)
    return vocab, a, b, z_lo, z_hi, core


def score_kernel(halves, bases, first, second, weights, wanted, stats):
    s = halves[0]
    nt = (((1,), (1,)), ((), ()))
    logits = lax.dot_general(weights[s], first[...], nt, preferred_element_type=jnp.float32)
    logits += lax.dot_general(weights[1 - s], second[...], nt, preferred_element_type=jnp.float32)
    cols = weights.shape[1] // 2
    label = wanted[...]
    own, other = label - bases[0], label - bases[1]
    row = jnp.where(
        (own >= 0) & (own < cols),
        own,
        jnp.where((other >= 0) & (other < cols), other + cols, -1),
    )
    peak = jnp.max(logits, axis=0, keepdims=True)
    total = jnp.sum(jnp.exp(logits - peak), axis=0, keepdims=True)
    at = lax.broadcasted_iota(jnp.int32, logits.shape, 0)
    picked = jnp.sum(jnp.where(at == row, logits, 0.0), axis=0, keepdims=True)
    stats[0:1, :] = peak + jnp.log(total)
    stats[1:2, :] = picked


def score(half, bases, first, second, weights, wanted):
    rows, depth = first.shape
    cols = weights.shape[1]
    vmem = pl.BlockSpec(memory_space=pltpu.VMEM)
    smem = pl.BlockSpec(memory_space=pltpu.SMEM)
    return pl.pallas_call(
        score_kernel,
        out_shape=jax.ShapeDtypeStruct((2, rows), jnp.float32),
        in_specs=[smem, smem, vmem, vmem, vmem, vmem],
        out_specs=vmem,
        compiler_params=pltpu.CompilerParams(vmem_limit_bytes=24 * 1024 * 1024),
        cost_estimate=pl.CostEstimate(
            flops=4 * rows * depth * cols, bytes_accessed=4 * rows * depth, transcendentals=rows * cols
        ),
        name="score",
    )(half, bases, first, second, weights, wanted)


def merged(stats, **axis):
    name = next(iter(axis))
    parts = [stats] + [pull(stats, **{name: shift}) for shift in (1, 2, 3)]
    logs = [part[0] for part in parts]
    peak = jnp.maximum(jnp.maximum(logs[0], logs[1]), jnp.maximum(logs[2], logs[3]))
    total = sum(jnp.exp(value - peak) for value in logs)
    return jnp.stack([peak + jnp.log(total), sum(part[1] for part in parts)])


def body(hidden, unembed, labels):
    vocab, a, b, z_lo, z_hi, core = place()
    tokens = labels.shape[0] // 2
    depth, cols = unembed.shape
    rows = hidden[0]
    keep = lax.dynamic_slice_in_dim(rows, core * tokens, tokens, 0)
    give = lax.dynamic_slice_in_dim(rows, (1 - core) * tokens, tokens, 0)
    got = pull(give, dc=1)
    unit = jnp.where(
        core == 0, jnp.concatenate([keep, got], 1), jnp.concatenate([got, keep], 1)
    )
    turned = jnp.swapaxes(unembed.reshape(2, depth // 2, cols), 1, 2)
    weights = jnp.concatenate([turned, pull(turned, dc=1)], 1)
    chip_first = (vocab * 4 + z_hi * 2) * cols
    bases = jnp.stack([chip_first + core * cols, chip_first + (1 - core) * cols])
    wide = jnp.broadcast_to(labels[None], (32, labels.shape[0]))
    all_labels = lax.all_to_all(wide, "vocab", 0, 0, tiled=True).reshape(64, tokens)
    steps = jnp.arange(4)
    db, odd, da = steps[:, None, None], jnp.arange(2)[None, :, None], steps[None, None, :]
    at_a, at_b = (a + da) % 4, (b + db) % 4
    at_x, at_y = jnp.where(core == 0, at_a, at_b), jnp.where(core == 0, at_b, at_a)
    block = (at_y * 4 + at_x) * 2 + (z_lo + odd) % 2
    wanted = jnp.take(all_labels, (block * 2 + core).reshape(-1), axis=0, mode="clip")
    wanted = wanted.reshape(4, 2, 1, 4 * tokens)
    line = jnp.concatenate([unit] + [pull(unit, da=shift) for shift in (1, 2, 3)], 0)
    part = line.shape[0] // 2
    up, down = pull(line, dz=1), pull(line, dz=-1)
    far = jnp.concatenate([pull(up[:part], dz=1), pull(down[part:], dz=-1)], 0)
    next_line, last_line = pull(line, db=1), pull(line, db=-1)
    across = pull(line, db=2)
    next_up, last_up = pull(up, db=1), pull(up, db=-1)
    next_down, last_down = pull(down, db=1), pull(down, db=-1)
    across_up, across_down = pull(across, dz=1), pull(across, dz=-1)
    next_far, last_far = pull(far, db=1), pull(far, db=-1)
    across_far = jnp.concatenate([pull(next_far[:part], db=1), pull(last_far[part:], db=-1)], 0)
    even = jnp.reshape(z_hi, (1,))
    odd_half = jnp.reshape(((z_hi * 2 + z_lo + 1) % 4) // 2, (1,))
    pairs = [
        [(line, far), (up, down)],
        [(next_line, next_far), (next_up, next_down)],
        [(across, across_far), (across_up, across_down)],
        [(last_line, last_far), (last_up, last_down)],
    ]
    found = [
        score((even, odd_half)[k], bases, *pairs[i][k], weights, wanted[i, k])
        for i in range(4)
        for k in range(2)
    ]
    ordered = jnp.stack(found, 1).reshape(2, 32, tokens)
    every = jnp.arange(32)
    to_x, to_y = (every // 2) % 4, every // 8
    to_a, to_b = jnp.where(core == 0, to_x, to_y), jnp.where(core == 0, to_y, to_x)
    where_at = (((to_b - b) % 4) * 2 + (every + z_lo) % 2) * 4 + (to_a - a) % 4
    stats = jnp.take(ordered, where_at, axis=1, mode="clip")
    for axis in ("da", "db", "dz"):
        stats = merged(stats, **{axis: 1})
    loss = stats[0] - stats[1]
    theirs = pull(loss, dc=1)
    both = jnp.where(core == 0, jnp.stack([loss, theirs], 1), jnp.stack([theirs, loss], 1))
    token_loss = both.reshape(1, -1)
    return token_loss, jnp.mean(token_loss, axis=1)


def solution(mesh):
    placed = (P(None, "vocab", "hid"), P(None, ("vocab", "hid")), P("vocab"))
    return jax.shard_map(body, mesh=mesh, in_specs=placed, out_specs=(P(), P()), check_vma=False)
```

```python
import jax
import jax.numpy as jnp
from jax import lax
from jax.experimental import pallas as pl
from jax.experimental.pallas import tpu as pltpu
from jax.sharding import PartitionSpec as P


AXES = ("vocab", "hid")


def device_number(y, x, z, core):
    return ((y * 4 + x) * 2 + z % 2) * 4 + (z // 2) * 2 + core


def source_pairs(da, db, dz, dc):
    pairs = []
    for y in range(4):
        for x in range(4):
            for z in range(4):
                for core in range(2):
                    dx, dy = (da, db) if core == 0 else (db, da)
                    source = device_number((y + dy) % 4, (x + dx) % 4, (z + dz) % 4, core ^ dc)
                    pairs.append((source, device_number(y, x, z, core)))
    return pairs


def pull(value, da=0, db=0, dz=0, dc=0):
    return lax.ppermute(value, AXES, source_pairs(da, db, dz, dc))


NT = (((1,), (1,)), ((), ()))


def half_kernel(here, *refs):
    weights, logits = refs[-2], refs[-1]
    first = jnp.concatenate([ref[...] for ref in refs[:-2]], 0)
    logits[...] = lax.dot_general(
        weights[here[1] >> 1], first, NT, preferred_element_type=jnp.float32
    )


def score_kernel(steps, odd, size, started, here, *refs):
    weights, labels, stats = refs[-7], refs[-6:-2], refs[-1]
    pieces = [ref[at : at + size] for ref in refs[started:-7] for at in range(0, ref.shape[0], size)]
    vocab, hid = here[0], here[1]
    y, x, z_lo = vocab >> 3, (vocab >> 1) & 3, vocab & 1
    z_hi, core = hid >> 1, hid & 1
    a, b = jnp.where(core == 0, x, y), jnp.where(core == 0, y, x)
    half = ((z_hi * 2 + z_lo + 1) & 3) >> 1 if odd else z_hi
    groups = labels[0].shape[1]
    blocks = []
    for db in steps:
        for da in range(4):
            at_a, at_b = (a + da) & 3, (b + db) & 3
            at_x, at_y = jnp.where(core == 0, at_a, at_b), jnp.where(core == 0, at_b, at_a)
            blocks.append((at_y * 4 + at_x) * 2 + ((z_lo + odd) & 1))
    if started:
        second = jnp.concatenate(pieces, 0)
        logits = refs[0][...]
    else:
        first, second = jnp.concatenate(pieces[0::2], 0), jnp.concatenate(pieces[1::2], 0)
        logits = lax.dot_general(weights[half], first, NT, preferred_element_type=jnp.float32)
    logits += lax.dot_general(weights[1 - half], second, NT, preferred_element_type=jnp.float32)
    cols = weights.shape[1] // 2
    chip_first = (vocab * 4 + z_hi * 2) * cols
    label = [labels[db][odd * 4 + da : odd * 4 + da + 1, :] for db in steps for da in range(4)]
    label = jnp.concatenate(label, 1)
    own = label - (chip_first + core * cols)
    other = label - (chip_first + (1 - core) * cols)
    row = jnp.where(
        (own >= 0) & (own < cols),
        own,
        jnp.where((other >= 0) & (other < cols), other + cols, -1),
    )
    peak = jnp.max(logits, axis=0, keepdims=True)
    total = jnp.sum(jnp.exp(logits - peak), axis=0, keepdims=True)
    column = lax.broadcasted_iota(jnp.int32, logits.shape, 0)
    picked = jnp.sum(jnp.where(column == row, logits, 0.0), axis=0, keepdims=True)
    soft = peak + jnp.log(total)
    for n, block in enumerate(blocks):
        part = slice(n * groups, (n + 1) * groups)
        stats[0, pl.ds(block, 1), :] = soft[:, part]
        stats[1, pl.ds(block, 1), :] = picked[:, part]


def turn_kernel(own, other, turned, chunks, sems):
    halves, depth, step = turned.shape[0], turned.shape[2], chunks.shape[1]
    cols = own.shape[1]
    pieces = depth // step

    def copy(source, k, slot):
        return pltpu.make_async_copy(
            source.at[pl.ds(pl.multiple_of(k * step, step), step), :], chunks.at[slot], sems.at[slot]
        )

    for side, source in enumerate((own, other)):
        copy(source, 0, 2 * side).start()

    @pl.loop(0, halves * pieces)
    def _(k):
        for side, source in enumerate((own, other)):
            slot = 2 * side + k % 2

            @pl.when(k + 1 < halves * pieces)
            def _():
                copy(source, k + 1, 2 * side + (k + 1) % 2).start()

            copy(source, k, slot).wait()
            at = pl.multiple_of((k % pieces) * step, step)
            turned[k // pieces, pl.ds(side * cols, cols), pl.ds(at, step)] = chunks[slot].T


def turn(own, other):
    depth, cols = own.shape
    step = 256
    hbm = pl.BlockSpec(memory_space=pltpu.HBM)
    return pl.pallas_call(
        turn_kernel,
        out_shape=jax.ShapeDtypeStruct((2, 2 * cols, depth // 2), own.dtype),
        in_specs=[hbm, hbm],
        out_specs=pl.BlockSpec(memory_space=pltpu.VMEM),
        scratch_shapes=[pltpu.VMEM((4, step, cols), own.dtype), pltpu.SemaphoreType.DMA((4,))],
        compiler_params=pltpu.CompilerParams(vmem_limit_bytes=VMEM_LIMIT),
        cost_estimate=pl.CostEstimate(
            flops=4 * depth * cols, bytes_accessed=8 * depth * cols, transcendentals=0
        ),
        name="turn",
    )(own, other)


def begin(here, parts, weights):
    rows = sum(part.shape[0] for part in parts)
    cols, depth = weights.shape[1:]
    vmem = pl.BlockSpec(memory_space=pltpu.VMEM)
    return pl.pallas_call(
        half_kernel,
        out_shape=jax.ShapeDtypeStruct((cols, rows), jnp.float32),
        in_specs=[pl.BlockSpec(memory_space=pltpu.SMEM)] + [vmem] * (len(parts) + 1),
        out_specs=vmem,
        compiler_params=pltpu.CompilerParams(vmem_limit_bytes=VMEM_LIMIT),
        cost_estimate=pl.CostEstimate(
            flops=2 * rows * depth * cols, bytes_accessed=2 * rows * depth, transcendentals=0
        ),
        name="begin",
    )(here, *parts, weights)


def score(steps, odd, here, parts, size, weights, labels, stats):
    cols, depth = weights.shape[1:]
    rows = size * len(steps)
    started = int(parts[0].dtype == jnp.float32)
    vmem = pl.BlockSpec(memory_space=pltpu.VMEM)

    def kernel(*refs):
        score_kernel(steps, odd, size, started, *refs)

    return pl.pallas_call(
        kernel,
        out_shape=jax.ShapeDtypeStruct(stats.shape, stats.dtype),
        in_specs=[pl.BlockSpec(memory_space=pltpu.SMEM)] + [vmem] * (len(parts) + 6),
        out_specs=vmem,
        input_output_aliases={len(parts) + 6: 0},
        compiler_params=pltpu.CompilerParams(vmem_limit_bytes=VMEM_LIMIT),
        cost_estimate=pl.CostEstimate(
            flops=2 * (2 - started) * rows * depth * cols,
            bytes_accessed=4 * rows * depth,
            transcendentals=rows * cols,
        ),
        name="score",
    )(here, *parts, weights, *labels, stats)


VMEM_LIMIT = 16 * 1024 * 1024


def merged(stats, **axis):
    key = next(iter(axis))
    parts = [stats] + [pull(stats, **{key: n}) for n in (1, 2, 3)]
    logs = [part[0] for part in parts]
    peak = jnp.maximum(jnp.maximum(logs[0], logs[1]), jnp.maximum(logs[2], logs[3]))
    total = sum(jnp.exp(value - peak) for value in logs)
    return jnp.stack([peak + jnp.log(total), sum(part[1] for part in parts)])


def losses(hidden, unembed, labels):
    vocab, hid = lax.axis_index("vocab"), lax.axis_index("hid")
    core = hid % 2
    here = jnp.stack([vocab, hid])
    tokens = labels.shape[0] // 2
    rows = hidden[0]
    keep = lax.dynamic_slice_in_dim(rows, core * tokens, tokens, 0)
    give = lax.dynamic_slice_in_dim(rows, (1 - core) * tokens, tokens, 0)
    got = pull(give, dc=1)
    unit = jnp.where(
        core == 0, jnp.concatenate([keep, got], 1), jnp.concatenate([got, keep], 1)
    )
    unit, here = lax.optimization_barrier((unit, here))
    weights = turn(unembed, pull(unembed, dc=1))
    known = jnp.stack([labels, pull(labels, dz=1)])
    known = lax.dynamic_slice_in_dim(known, core * tokens, tokens, 1)
    known = jnp.stack([known] + [pull(known, da=n) for n in (1, 2, 3)], 1)
    known = known.reshape(8, tokens)
    known = [known] + [pull(known, db=n) for n in (1, 2, 3)]
    line = jnp.concatenate([unit] + [pull(unit, da=n) for n in (1, 2, 3)], 0)
    size = line.shape[0]
    part = size // 2
    up, down = pull(line, dz=1), pull(line, dz=-1)
    next_line, last_line = pull(line, db=1), pull(line, db=-1)
    across = pull(line, db=2)
    both = jnp.concatenate([up, down], 0)
    next_both, last_both = pull(both, db=1), pull(both, db=-1)
    far = jnp.concatenate([pull(up[:part], dz=1), pull(down[part:], dz=-1)], 0)
    across_up, across_down = pull(across, dz=1), pull(across, dz=-1)
    next_far, last_far = pull(far, db=1), pull(far, db=-1)
    across_far = jnp.concatenate([pull(next_far[:part], db=1), pull(last_far[part:], db=-1)], 0)
    nearby = begin(here, (next_line, last_line), weights)
    distant = begin(here, (across,), weights)
    work = [
        ((0,), 1, (up, down)),
        ((0,), 0, (line, far)),
        ((1,), 1, (next_both,)),
        ((3,), 1, (last_both,)),
        ((1, 3), 0, (nearby, next_far, last_far)),
        ((2,), 1, (across_up, across_down)),
        ((2,), 0, (distant, across_far)),
    ]
    stats = jnp.zeros((2, 32, tokens), jnp.float32)
    for steps, odd, parts in work:
        stats = score(steps, odd, here, parts, size, weights, known, stats)
    for axis in ("da", "db", "dz"):
        stats = merged(stats, **{axis: 1})
    loss = stats[0] - stats[1]
    theirs = pull(loss, dc=1)
    token_loss = jnp.where(
        core == 0, jnp.concatenate([loss, theirs], 1), jnp.concatenate([theirs, loss], 1)
    ).reshape(1, -1)
    return token_loss, jnp.mean(token_loss, axis=1)


def solution(mesh):
    placed = (P(None, "vocab", "hid"), P(None, ("vocab", "hid")), P("vocab"))
    return jax.shard_map(losses, mesh=mesh, in_specs=placed, out_specs=(P(), P()), check_vma=False)
```

```python
import jax
import jax.numpy as jnp
from jax import lax
from jax.experimental import pallas as pl
from jax.experimental.pallas import tpu as pltpu
from jax.sharding import PartitionSpec as P


AXES = ("vocab", "hid")


def device_number(y, x, z, core):
    return ((y * 4 + x) * 2 + z % 2) * 4 + (z // 2) * 2 + core


def source_pairs(da, db, dz, dc):
    pairs = []
    for y in range(4):
        for x in range(4):
            for z in range(4):
                for core in range(2):
                    dx, dy = (da, db) if core == 0 else (db, da)
                    source = device_number((y + dy) % 4, (x + dx) % 4, (z + dz) % 4, core ^ dc)
                    pairs.append((source, device_number(y, x, z, core)))
    return pairs


def pull(value, da=0, db=0, dz=0, dc=0):
    return lax.ppermute(value, AXES, source_pairs(da, db, dz, dc))


NT = (((1,), (1,)), ((), ()))


def half_kernel(here, *refs):
    weights, logits = refs[-2], refs[-1]
    first = jnp.concatenate([ref[...] for ref in refs[:-2]], 0)
    logits[...] = lax.dot_general(
        weights[here[1] >> 1], first, NT, preferred_element_type=jnp.float32
    )


def score_kernel(steps, odd, size, started, here, *refs):
    weights, labels, stats = refs[-7], refs[-6:-2], refs[-1]
    pieces = [
        ref[at : min(at + size, ref.shape[0])]
        for ref in refs[started:-7]
        for at in range(0, ref.shape[0], size)
    ]
    vocab, hid = here[0], here[1]
    y, x, z_lo = vocab >> 3, (vocab >> 1) & 3, vocab & 1
    z_hi, core = hid >> 1, hid & 1
    a, b = jnp.where(core == 0, x, y), jnp.where(core == 0, y, x)
    half = ((z_hi * 2 + z_lo + 1) & 3) >> 1 if odd else z_hi
    groups = labels[0].shape[1]
    blocks = []
    for db in steps:
        for da in range(4):
            at_a, at_b = (a + da) & 3, (b + db) & 3
            at_x, at_y = jnp.where(core == 0, at_a, at_b), jnp.where(core == 0, at_b, at_a)
            blocks.append((at_y * 4 + at_x) * 2 + ((z_lo + odd) & 1))
    if started:
        second = jnp.concatenate(pieces, 0)
        logits = refs[0][...]
    else:
        first, second = jnp.concatenate(pieces[0::2], 0), jnp.concatenate(pieces[1::2], 0)
        logits = lax.dot_general(weights[half], first, NT, preferred_element_type=jnp.float32)
    logits += lax.dot_general(weights[1 - half], second, NT, preferred_element_type=jnp.float32)
    cols = weights.shape[1] // 2
    chip_first = (vocab * 4 + z_hi * 2) * cols
    label = [labels[db][odd * 4 + da : odd * 4 + da + 1, :] for db in steps for da in range(4)]
    label = jnp.concatenate(label, 1)
    own = label - (chip_first + core * cols)
    other = label - (chip_first + (1 - core) * cols)
    row = jnp.where(
        (own >= 0) & (own < cols),
        own,
        jnp.where((other >= 0) & (other < cols), other + cols, -1),
    )
    peak = jnp.max(logits, axis=0, keepdims=True)
    total = jnp.sum(jnp.exp(logits - peak), axis=0, keepdims=True)
    column = lax.broadcasted_iota(jnp.int32, logits.shape, 0)
    picked = jnp.sum(jnp.where(column == row, logits, 0.0), axis=0, keepdims=True)
    soft = peak + jnp.log(total)
    for n, block in enumerate(blocks):
        part = slice(n * groups, (n + 1) * groups)
        stats[0, pl.ds(block, 1), :] = soft[:, part]
        stats[1, pl.ds(block, 1), :] = picked[:, part]


def turn_kernel(own, other, turned, chunks, sems):
    halves, depth, step = turned.shape[0], turned.shape[2], chunks.shape[1]
    cols = own.shape[1]
    pieces = depth // step

    def copy(source, k, slot):
        return pltpu.make_async_copy(
            source.at[pl.ds(pl.multiple_of(k * step, step), step), :], chunks.at[slot], sems.at[slot]
        )

    for side, source in enumerate((own, other)):
        copy(source, 0, 2 * side).start()

    @pl.loop(0, halves * pieces)
    def _(k):
        for side, source in enumerate((own, other)):
            slot = 2 * side + k % 2

            @pl.when(k + 1 < halves * pieces)
            def _():
                copy(source, k + 1, 2 * side + (k + 1) % 2).start()

            copy(source, k, slot).wait()
            at = pl.multiple_of((k % pieces) * step, step)
            turned[k // pieces, pl.ds(side * cols, cols), pl.ds(at, step)] = chunks[slot].T


def turn(own, other):
    depth, cols = own.shape
    step = 896
    hbm = pl.BlockSpec(memory_space=pltpu.HBM)
    return pl.pallas_call(
        turn_kernel,
        out_shape=jax.ShapeDtypeStruct((2, 2 * cols, depth // 2), own.dtype),
        in_specs=[hbm, hbm],
        out_specs=pl.BlockSpec(memory_space=pltpu.VMEM),
        scratch_shapes=[pltpu.VMEM((4, step, cols), own.dtype), pltpu.SemaphoreType.DMA((4,))],
        compiler_params=pltpu.CompilerParams(vmem_limit_bytes=VMEM_LIMIT),
        cost_estimate=pl.CostEstimate(
            flops=4 * depth * cols, bytes_accessed=8 * depth * cols, transcendentals=0
        ),
        name="turn",
    )(own, other)


def begin(here, parts, weights):
    rows = sum(part.shape[0] for part in parts)
    cols, depth = weights.shape[1:]
    vmem = pl.BlockSpec(memory_space=pltpu.VMEM)
    return pl.pallas_call(
        half_kernel,
        out_shape=jax.ShapeDtypeStruct((cols, rows), jnp.float32),
        in_specs=[pl.BlockSpec(memory_space=pltpu.SMEM)] + [vmem] * (len(parts) + 1),
        out_specs=vmem,
        compiler_params=pltpu.CompilerParams(vmem_limit_bytes=VMEM_LIMIT),
        cost_estimate=pl.CostEstimate(
            flops=2 * rows * depth * cols, bytes_accessed=2 * rows * depth, transcendentals=0
        ),
        name="begin",
    )(here, *parts, weights)


def score(steps, odd, here, parts, size, weights, labels, stats):
    cols, depth = weights.shape[1:]
    rows = size * len(steps)
    started = int(parts[0].dtype == jnp.float32)
    vmem = pl.BlockSpec(memory_space=pltpu.VMEM)

    def kernel(*refs):
        score_kernel(steps, odd, size, started, *refs)

    return pl.pallas_call(
        kernel,
        out_shape=jax.ShapeDtypeStruct(stats.shape, stats.dtype),
        in_specs=[pl.BlockSpec(memory_space=pltpu.SMEM)] + [vmem] * (len(parts) + 6),
        out_specs=vmem,
        input_output_aliases={len(parts) + 6: 0},
        compiler_params=pltpu.CompilerParams(vmem_limit_bytes=VMEM_LIMIT),
        cost_estimate=pl.CostEstimate(
            flops=2 * (2 - started) * rows * depth * cols,
            bytes_accessed=4 * rows * depth,
            transcendentals=rows * cols,
        ),
        name="score",
    )(here, *parts, weights, *labels, stats)


VMEM_LIMIT = 16 * 1024 * 1024


def merged(stats, **axis):
    key = next(iter(axis))
    parts = [stats] + [pull(stats, **{key: n}) for n in (1, 2, 3)]
    logs = [part[0] for part in parts]
    peak = jnp.maximum(jnp.maximum(logs[0], logs[1]), jnp.maximum(logs[2], logs[3]))
    total = sum(jnp.exp(value - peak) for value in logs)
    return jnp.stack([peak + jnp.log(total), sum(part[1] for part in parts)])


def losses(hidden, unembed, labels):
    vocab, hid = lax.axis_index("vocab"), lax.axis_index("hid")
    core = hid % 2
    here = jnp.stack([vocab, hid])
    tokens = labels.shape[0] // 2
    rows = hidden[0]
    keep = lax.dynamic_slice_in_dim(rows, core * tokens, tokens, 0)
    give = lax.dynamic_slice_in_dim(rows, (1 - core) * tokens, tokens, 0)
    got = pull(give, dc=1)
    unit = jnp.where(
        core == 0, jnp.concatenate([keep, got], 1), jnp.concatenate([got, keep], 1)
    )
    unit, here = lax.optimization_barrier((unit, here))
    weights = turn(unembed, pull(unembed, dc=1))
    known = jnp.stack([labels, pull(labels, dz=1)])
    known = lax.dynamic_slice_in_dim(known, core * tokens, tokens, 1)
    known = jnp.stack([known] + [pull(known, da=n) for n in (1, 2, 3)], 1)
    known = known.reshape(8, tokens)
    known = [known] + [pull(known, db=n) for n in (1, 2, 3)]
    line = jnp.concatenate([unit] + [pull(unit, da=n) for n in (1, 2, 3)], 0)
    size = line.shape[0]
    part = size // 2
    up, down = pull(line, dz=1), pull(line, dz=-1)
    next_line, last_line = pull(line, db=1), pull(line, db=-1)
    across = pull(line, db=2)
    both = jnp.concatenate([up, down], 0)
    next_both, last_both = pull(both, db=1), pull(both, db=-1)
    far = pull(up[:part], dz=1), pull(down[part:], dz=-1)
    across_up, across_down = pull(across, dz=1), pull(across, dz=-1)
    next_far = pull(far[0], db=1), pull(far[1], db=1)
    last_far = pull(far[0], db=-1), pull(far[1], db=-1)
    across_far = pull(next_far[0], db=1), pull(last_far[1], db=-1)
    here_half = begin(here, (line,), weights)
    nearby = begin(here, (next_line, last_line), weights)
    distant = begin(here, (across,), weights)
    work = [
        ((0,), 1, (up, down)),
        ((0,), 0, (here_half, *far)),
        ((1,), 1, (next_both,)),
        ((3,), 1, (last_both,)),
        ((2,), 1, (across_up, across_down)),
        ((1, 3), 0, (nearby, *next_far, *last_far)),
        ((2,), 0, (distant, *across_far)),
    ]
    stats = jnp.zeros((2, 32, tokens), jnp.float32)
    for steps, odd, parts in work:
        stats = score(steps, odd, here, parts, size, weights, known, stats)
    for axis in ("db", "da", "dz"):
        stats = merged(stats, **{axis: 1})
    loss = stats[0] - stats[1]
    theirs = pull(loss, dc=1)
    token_loss = jnp.where(
        core == 0, jnp.concatenate([loss, theirs], 1), jnp.concatenate([theirs, loss], 1)
    ).reshape(1, -1)
    return token_loss, jnp.mean(token_loss, axis=1)


def solution(mesh):
    placed = (P(None, "vocab", "hid"), P(None, ("vocab", "hid")), P("vocab"))
    return jax.shard_map(losses, mesh=mesh, in_specs=placed, out_specs=(P(), P()), check_vma=False)
```
